32 devices in a mesh: dp: 1 (over z), tp: 4 (over y), wg: 8 (over x, core).
Axes of the slice: x: 4, y: 4, z: 1, core: 2. Of those that a mesh axis runs over, the one named last changes fastest.
The devices are a block of a 4x4x8 slice.
Arguments:
- x_in: bfloat16 [16, 2048, 2048], P(('dp', 'wg'))
- valid: int32 [16, 2048], P(('dp', 'wg'))
- ln_gain: float32 [2048], replicated
- w_q: bfloat16 [2048, 2048], P('wg', 'tp')
- w_kv: bfloat16 [2048, 512], P('wg')
- w_gate: bfloat16 [2048, 16384], P('wg', 'tp')
- w_up: bfloat16 [2048, 16384], P('wg', 'tp')
- w_o: bfloat16 [2048, 2048], P('tp', 'wg')
- w_down: bfloat16 [16384, 2048], P('tp', 'wg')
Outputs:
- output 1: bfloat16 [16, 2048, 2048], P(('dp', 'wg'))
- output 2: bfloat16 [16, 2048, 256], P(('dp', 'wg'))
- output 3: bfloat16 [16, 2048, 256], P(('dp', 'wg'))
All inputs are finite; a program needn't handle non-finite values.
Results may differ from the reference program's by a relative error of at most 0.0137817.
Values are sent between devices in bfloat16 or wider.
A program may use at most 768 MiB of HBM per device.

```python
import jax
import jax.numpy as jnp
from jax import lax

D_MODEL = 2048
N_HEADS = 8
HEAD_DIM = 256
FF_DIM = 16384
BATCH_DEV = 2
SEQ_LEN = 2048
TP_SIZE = 4
WG_SIZE = 8

BATCH = BATCH_DEV * WG_SIZE
Q_COLS = N_HEADS * HEAD_DIM
ATTN_GAIN = (SEQ_LEN / 16) ** 0.5


def setup_inputs(seed: int = 0, part: int = 0) -> dict:
    key = jax.random.key(seed)
    part_keys = jax.random.split(jax.random.fold_in(key, part), 2)
    weight_keys = jax.random.split(jax.random.key(seed + 1), 7)
    x_in = (0.5 * jax.random.normal(part_keys[0], (BATCH, SEQ_LEN, D_MODEL), jnp.float32)).astype(jnp.bfloat16)
    lengths = jax.random.randint(part_keys[1], (BATCH,), 1, SEQ_LEN + 1).at[0].set(SEQ_LEN)
    valid = (jnp.arange(SEQ_LEN)[None, :] < lengths[:, None]).astype(jnp.int32)
    ln_gain = 1.0 + 0.3 * jax.random.normal(weight_keys[0], (D_MODEL,), jnp.float32)

    def draw(sub_key, shape, scale):
        return (jax.random.normal(sub_key, shape, jnp.float32) * scale).astype(jnp.bfloat16)

    return {'x_in': x_in, 'valid': valid, 'ln_gain': ln_gain,
            'w_q': draw(weight_keys[1], (D_MODEL, Q_COLS), D_MODEL ** -0.5),
            'w_kv': draw(weight_keys[2], (D_MODEL, 2 * HEAD_DIM), D_MODEL ** -0.5),
            'w_gate': draw(weight_keys[3], (D_MODEL, FF_DIM), D_MODEL ** -0.5),
            'w_up': draw(weight_keys[4], (D_MODEL, FF_DIM), D_MODEL ** -0.5),
            'w_o': draw(weight_keys[5], (Q_COLS, D_MODEL), ATTN_GAIN * Q_COLS ** -0.5),
            'w_down': draw(weight_keys[6], (FF_DIM, D_MODEL), FF_DIM ** -0.5)}


def rope_tables(seq_len, head_dim):
    half = head_dim // 2
    inv_freq = 10000.0 ** (-2.0 * jnp.arange(half, dtype=jnp.float32) / head_dim)
    angles = jnp.arange(seq_len, dtype=jnp.float32)[:, None] * inv_freq[None, :]
    return jnp.cos(angles), jnp.sin(angles)


def apply_rope(vals, cos_t, sin_t):
    half = vals.shape[-1] // 2
    first = vals[..., :half]
    second = vals[..., half:]
    return jnp.concatenate([first * cos_t - second * sin_t, second * cos_t + first * sin_t], axis=-1)


def reference(x_in, valid, ln_gain, w_q, w_kv, w_gate, w_up, w_o, w_down):
    cos_t, sin_t = rope_tables(SEQ_LEN, HEAD_DIM)
    positions = jnp.arange(SEQ_LEN)
    causal = positions[None, :] <= positions[:, None]
    wo_parts = w_o.astype(jnp.float32).reshape(TP_SIZE, Q_COLS // TP_SIZE, D_MODEL)
    wd_parts = w_down.astype(jnp.float32).reshape(TP_SIZE, FF_DIM // TP_SIZE, D_MODEL)

    def one_prompt(item):
        rows, mask_row = item
        x_f32 = rows.astype(jnp.float32)
        mean = x_f32.mean(axis=-1, keepdims=True)
        centered = x_f32 - mean
        x_var = (centered * centered).mean(axis=-1, keepdims=True)
        normed = (centered * lax.rsqrt(x_var + 1e-6) * ln_gain).astype(jnp.bfloat16)
        q_proj = jnp.dot(normed, w_q, preferred_element_type=jnp.float32).astype(jnp.bfloat16)
        kv_proj = jnp.dot(normed, w_kv, preferred_element_type=jnp.float32).astype(jnp.bfloat16)
        gate_proj = jnp.dot(normed, w_gate, preferred_element_type=jnp.float32).astype(jnp.bfloat16)
        up_proj = jnp.dot(normed, w_up, preferred_element_type=jnp.float32).astype(jnp.bfloat16)
        q_heads = q_proj.reshape(SEQ_LEN, N_HEADS, HEAD_DIM).astype(jnp.float32)
        q_rot = apply_rope(q_heads, cos_t[:, None, :], sin_t[:, None, :]).astype(jnp.bfloat16)
        k_rot = apply_rope(kv_proj[:, :HEAD_DIM].astype(jnp.float32), cos_t, sin_t).astype(jnp.bfloat16)
        v_rows = kv_proj[:, HEAD_DIM:]
        scores = jnp.einsum('she,te->hst', q_rot.astype(jnp.float32), k_rot.astype(jnp.float32)) * HEAD_DIM ** -0.5
        allowed = causal & (mask_row[None, :] > 0)
        scores = jnp.where(allowed[None], scores, -1e30)
        probs = jax.nn.softmax(scores, axis=-1).astype(jnp.bfloat16)
        attn_out = jnp.einsum('hst,te->she', probs.astype(jnp.float32), v_rows.astype(jnp.float32)).astype(jnp.bfloat16)
        mlp_out = (jax.nn.silu(gate_proj.astype(jnp.float32)) * up_proj.astype(jnp.float32)).astype(jnp.bfloat16)
        attn_parts = attn_out.reshape(SEQ_LEN, TP_SIZE, Q_COLS // TP_SIZE).astype(jnp.float32)
        mlp_parts = mlp_out.reshape(SEQ_LEN, TP_SIZE, FF_DIM // TP_SIZE).astype(jnp.float32)
        partials = (jnp.einsum('sjk,jkd->sjd', attn_parts, wo_parts) + jnp.einsum('sjk,jkd->sjd', mlp_parts, wd_parts)).astype(jnp.bfloat16)
        out_rows = (x_f32 + partials.astype(jnp.float32).sum(axis=1)).astype(jnp.bfloat16)
        keep = mask_row[:, None] > 0
        return out_rows, jnp.where(keep, k_rot, 0), jnp.where(keep, v_rows, 0)

    y_out, k_cache, v_cache = lax.map(one_prompt, (x_in, valid))
    return (y_out, k_cache, v_cache)
```

```python
import functools

import jax
import jax.numpy as jnp
from jax import lax
from jax.experimental import pallas as pl
from jax.experimental.pallas import tpu as pltpu
from jax.sharding import PartitionSpec as P


F32 = jnp.float32
BF16 = jnp.bfloat16
N_PIECES = 8
FF_TILE = 512
VMEM_LIMIT = 60 * 1024 * 1024


def after(val, *deps):
    return lax.optimization_barrier((val,) + deps)[0]


def params(sem):
    return pltpu.CompilerParams(dimension_semantics=sem, vmem_limit_bytes=VMEM_LIMIT)


def cost(flops, nbytes):
    return pl.CostEstimate(flops=int(flops), bytes_accessed=int(nbytes), transcendentals=0)


def ln_kernel(pos_ref, x_ref, gain_ref, z_ref):
    sub = 32
    blk = x_ref.shape[1] // N_PIECES

    def body(i, carry):
        rows = pl.ds(pl.multiple_of(i * sub, sub), sub)
        x = x_ref[rows, :].astype(F32)
        mean = jnp.mean(x, axis=-1, keepdims=True)
        cen = x - mean
        var = jnp.mean(cen * cen, axis=-1, keepdims=True)
        z = (cen * lax.rsqrt(var + 1e-6) * gain_ref[...]).astype(BF16)
        for j in range(N_PIECES):
            z_ref[rows, pl.ds(pl.multiple_of(pos_ref[j] * blk, blk), blk)] = z[:, j * blk:(j + 1) * blk]
        return carry

    lax.fori_loop(0, x_ref.shape[0] // sub, body, 0, unroll=2)


def layer_norm(x, gain, pos, prompt, seq):
    dim = x.shape[1]
    tm = 512
    n_m = seq // tm
    return pl.pallas_call(
        ln_kernel,
        grid_spec=pltpu.PrefetchScalarGridSpec(
            num_scalar_prefetch=1, grid=(n_m,),
            in_specs=[pl.BlockSpec((tm, dim), lambda i, p: (prompt * n_m + i, 0)),
                      pl.BlockSpec((1, dim), lambda i, p: (0, 0))],
            out_specs=pl.BlockSpec((tm, dim), lambda i, p: (i, 0))),
        out_shape=jax.ShapeDtypeStruct((seq, dim), BF16),
        compiler_params=params(("arbitrary",)),
        cost_estimate=cost(5e9, seq * dim * 4),
        name="ln",
    )(pos, x, gain.reshape(1, dim))


def fill_rows(w_s, pieces, col=0):
    row = 0
    for p in pieces:
        w_s[pl.ds(row, p.shape[0]), pl.ds(col, p.shape[1])] = p[...]
        row += p.shape[0]


def apply_rope(vals, cos_t, sin_t):
    half = vals.shape[-1] // 2
    a, b = vals[:, :half], vals[:, half:]
    return a * cos_t - b * sin_t, b * cos_t + a * sin_t


def qkv_kernel(n_heads, hd, aliased, *refs):
    z_ref, cos_ref, sin_ref, valid_ref = refs[:4]
    pieces = refs[4:-5 - aliased]
    q_ref, k_ref, v_ref, vr_ref, w_s = refs[-5:]

    @pl.when(pl.program_id(0) == 0)
    def _():
        fill_rows(w_s, pieces)

    half = hd // 2
    sub = 256
    for r in range(0, z_ref.shape[0], sub):
        rows = pl.ds(r, sub)
        out = jnp.dot(z_ref[rows, :], w_s[...], preferred_element_type=F32).astype(BF16)
        cos_t, sin_t = cos_ref[rows, :], sin_ref[rows, :]
        keep = valid_ref[rows, :] > 0
        for h in range(n_heads):
            a, b = apply_rope(out[:, h * hd:(h + 1) * hd].astype(F32), cos_t, sin_t)
            q_ref[rows, h * hd:h * hd + half] = a.astype(BF16)
            q_ref[rows, h * hd + half:(h + 1) * hd] = b.astype(BF16)
        base = n_heads * hd
        a, b = apply_rope(out[:, base:base + hd].astype(F32), cos_t, sin_t)
        k_ref[rows, :half] = jnp.where(keep, a, 0.0).astype(BF16)
        k_ref[rows, half:] = jnp.where(keep, b, 0.0).astype(BF16)
        v = out[:, base + hd:]
        vr_ref[rows, :] = v
        v_ref[rows, :] = jnp.where(keep, v.astype(F32), 0.0).astype(BF16)


def qkv(z, pieces, cos_t, sin_t, valid_col, hd, prompt, caches):
    seq, dim = z.shape
    rows = valid_col.shape[0]
    cols = pieces[0].shape[1]
    n_heads = cols // hd - 2
    tm = 1024
    n_m = seq // tm
    full = lambda p: pl.BlockSpec(p.shape, lambda i: (0, 0))
    ops = [z, cos_t, sin_t, valid_col] + list(pieces) + list(caches)
    at = len(ops) - len(caches)
    cache_spec = pl.BlockSpec((tm, hd), lambda i: (prompt * n_m + i, 0))
    return pl.pallas_call(
        functools.partial(qkv_kernel, n_heads, hd, len(caches)),
        grid=(n_m,),
        in_specs=[pl.BlockSpec((tm, dim), lambda i: (i, 0)),
                  pl.BlockSpec((tm, hd // 2), lambda i: (i, 0)),
                  pl.BlockSpec((tm, hd // 2), lambda i: (i, 0)),
                  pl.BlockSpec((tm, 1), lambda i: (prompt * n_m + i, 0))] + [full(p) for p in pieces]
        + [pl.BlockSpec(memory_space=pl.ANY)] * len(caches),
        out_specs=[pl.BlockSpec((tm, n_heads * hd), lambda i: (i, 0)), cache_spec, cache_spec,
                   pl.BlockSpec((tm, hd), lambda i: (i, 0))],
        out_shape=[jax.ShapeDtypeStruct((seq, n_heads * hd), BF16)] + [jax.ShapeDtypeStruct((rows, hd), BF16)] * 2
        + [jax.ShapeDtypeStruct((seq, hd), BF16)],
        scratch_shapes=[pltpu.VMEM((dim, cols), BF16)],
        input_output_aliases={at + i: 1 + i for i in range(len(caches))},
        compiler_params=params(("arbitrary",)),
        cost_estimate=cost(2 * seq * dim * cols, seq * dim * 4),
        name="qkv",
    )(*ops)


def attn_kernel(n_blk, scale, q_ref, k_ref, v_ref, valid_ref, o_ref):
    i = pl.program_id(1)
    blk = q_ref.shape[0]
    dn = (((1,), (1,)), ((), ()))

    def block(b):
        past = b * blk
        q = q_ref[...]
        s1 = lax.dot_general(q, k_ref[past:past + blk, :], dn, preferred_element_type=F32) * scale
        rows = lax.broadcasted_iota(jnp.int32, (blk, blk), 0)
        cols = lax.broadcasted_iota(jnp.int32, (blk, blk), 1)
        ok1 = jnp.logical_and(cols <= rows, valid_ref[:, past:past + blk] > 0)
        s1 = jnp.where(ok1, s1, -1e30)
        top = jnp.max(s1, axis=-1, keepdims=True)
        if b:
            s0 = lax.dot_general(q, k_ref[:past, :], dn, preferred_element_type=F32) * scale
            s0 = jnp.where(valid_ref[:, :past] > 0, s0, -1e30)
            top = jnp.maximum(top, jnp.max(s0, axis=-1, keepdims=True))
            e0 = jnp.exp(s0 - top)
        e1 = jnp.exp(s1 - top)
        tot = jnp.sum(e1, axis=-1, keepdims=True)
        if b:
            tot = tot + jnp.sum(e0, axis=-1, keepdims=True)
        inv = 1.0 / tot
        out = jnp.dot((e1 * inv).astype(BF16), v_ref[past:past + blk, :], preferred_element_type=F32)
        if b:
            out = out + jnp.dot((e0 * inv).astype(BF16), v_ref[:past, :], preferred_element_type=F32)
        o_ref[...] = out.astype(BF16)

    for b in range(n_blk):
        pl.when(i == b)(functools.partial(block, b))


def attention(q, k, v, valid_row, prompt, act_cols):
    seq, hd = v.shape
    n_heads = q.shape[1] // hd
    blk = 512
    n_blk = seq // blk
    return pl.pallas_call(
        functools.partial(attn_kernel, n_blk, hd ** -0.5),
        grid=(n_heads, n_blk),
        in_specs=[pl.BlockSpec((blk, hd), lambda h, i: (i, h)),
                  pl.BlockSpec((seq, hd), lambda h, i: (prompt, 0)),
                  pl.BlockSpec((seq, hd), lambda h, i: (0, 0)),
                  pl.BlockSpec((None, 1, seq), lambda h, i: (prompt, 0, 0))],
        out_specs=pl.BlockSpec((blk, hd), lambda h, i: (i, h)),
        out_shape=jax.ShapeDtypeStruct((seq, act_cols), BF16),
        compiler_params=params(("arbitrary", "arbitrary")),
        cost_estimate=cost(16e9, seq * hd * 12),
        name="attn",
    )(q, k, v, valid_row)


def gu_kernel(*refs):
    z_ref = refs[0]
    pieces = refs[1:-3]
    m_ref, w_s = refs[-2:]

    @pl.when(pl.program_id(1) == 0)
    def _():
        fill_rows(w_s, pieces[:len(pieces) // 2])
        fill_rows(w_s, pieces[len(pieces) // 2:], w_s.shape[1] // 2)

    t = m_ref.shape[1]
    sub = 256
    for r in range(0, z_ref.shape[0], sub):
        rows = pl.ds(r, sub)
        out = jnp.dot(z_ref[rows, :], w_s[...], preferred_element_type=F32).astype(BF16)
        a = out[:, :t].astype(F32)
        u = out[:, t:].astype(F32)
        m_ref[rows, :] = (a * jax.nn.sigmoid(a) * u).astype(BF16)


def gate_up(z, pieces, act, first_col, lo=0, hi=None):
    seq, dim = z.shape
    n_tiles = pieces[0].shape[1] // (2 * FF_TILE)
    hi = n_tiles if hi is None else hi
    cols = (hi - lo) * 2 * FF_TILE
    tm = 1024
    first = first_col // FF_TILE + lo
    ops = [z] + list(pieces) + list(pieces) + [act]
    return pl.pallas_call(
        gu_kernel,
        grid=(cols // (2 * FF_TILE), seq // tm),
        in_specs=[pl.BlockSpec((tm, dim), lambda n, m: (m, 0))]
        + [pl.BlockSpec((p.shape[0], FF_TILE), lambda n, m: (0, lo + n)) for p in pieces]
        + [pl.BlockSpec((p.shape[0], FF_TILE), lambda n, m: (0, n_tiles + lo + n)) for p in pieces]
        + [pl.BlockSpec(memory_space=pl.ANY)],
        out_specs=pl.BlockSpec((tm, FF_TILE), lambda n, m: (m, first + n)),
        out_shape=jax.ShapeDtypeStruct(act.shape, BF16),
        scratch_shapes=[pltpu.VMEM((dim, 2 * FF_TILE), BF16)],
        input_output_aliases={len(ops) - 1: 0},
        compiler_params=params(("arbitrary", "arbitrary")),
        cost_estimate=cost(2 * seq * dim * cols, seq * dim * 4),
        name="gate_up",
    )(*ops)


def down_kernel(plan, act_ref, *refs):
    n_w = sum(len(p) for p in plan)
    w_refs = refs[:n_w]
    out_ref, w_s, sems = refs[-3:]
    j, m = pl.program_id(0), pl.program_id(1)

    def copies(t):
        at = sum(len(p) for p in plan[:t])
        slot = t % 2
        return [pltpu.make_async_copy(w_refs[at + i], w_s.at[slot, pl.ds(row, w_refs[at + i].shape[0]), pl.ds(col, w_refs[at + i].shape[1])],
                                      sems.at[slot, i]) for i, (row, col) in enumerate(plan[t])]

    for t in range(len(plan)):
        @pl.when(jnp.logical_and(j == t, m == 0))
        def _(t=t):
            if t == 0:
                for c in copies(0):
                    c.start()
            for c in copies(t):
                c.wait()
            if t + 1 < len(plan):
                for c in copies(t + 1):
                    c.start()

    slot = lax.rem(j, 2)
    sub = 256
    for r in range(0, out_ref.shape[0], sub):
        rows = pl.ds(r, sub)
        out_ref[rows, :] = jnp.dot(act_ref[rows, :], w_s[slot], preferred_element_type=F32).astype(BF16)


def down(act, pairs, n_cols=None, first=0, buf=None):
    seq, kdim = act.shape
    blk = pairs[0][0][0].shape[1]
    tm = 512
    plan, ws = [], []
    for pair in pairs:
        spots = []
        for side, group in enumerate(pair):
            row = 0
            for p in group:
                spots.append((row, side * blk))
                ws.append(p)
                row += p.shape[0]
        plan.append(spots)
    n_cols = n_cols or 2 * blk * len(pairs)
    aliased = 0 if buf is None else 1
    ops = [act] + ws + ([buf] if aliased else [])
    return pl.pallas_call(
        functools.partial(down_kernel, plan),
        grid=(len(pairs), seq // tm),
        in_specs=[pl.BlockSpec((tm, kdim), lambda j, m: (m, 0))] + [pl.BlockSpec(memory_space=pl.ANY)] * (len(ws) + aliased),
        out_specs=pl.BlockSpec((tm, 2 * blk), lambda j, m: (m, first + j)),
        out_shape=jax.ShapeDtypeStruct((seq, n_cols), BF16),
        scratch_shapes=[pltpu.VMEM((2, kdim, 2 * blk), BF16), pltpu.SemaphoreType.DMA((2, 4))],
        input_output_aliases={len(ops) - 1: 0} if aliased else {},
        compiler_params=params(("arbitrary", "arbitrary")),
        cost_estimate=cost(2 * seq * kdim * 2 * blk * len(pairs), seq * kdim * 2),
        name="down",
    )(*ops)


def add_kernel(n_tot, idx_ref, x_ref, *refs):
    tots, y_ref = refs[:n_tot], refs[-1]
    blk = x_ref.shape[1] // N_PIECES
    j = 0
    for t in tots:
        for c in range(0, t.shape[1], blk):
            spot = pl.ds(pl.multiple_of(idx_ref[j] * blk, blk), blk)
            y_ref[:, spot] = (x_ref[:, spot].astype(F32) + t[:, c:c + blk].astype(F32)).astype(BF16)
            j += 1


def residual(x, totals, idx, y, prompt, seq):
    rows, dim = x.shape
    tm = 512
    n_m = seq // tm
    aliased = 0 if y is None else 1
    spot = lambda m, p: (prompt * n_m + m, 0)
    return pl.pallas_call(
        functools.partial(add_kernel, len(totals)),
        grid_spec=pltpu.PrefetchScalarGridSpec(
            num_scalar_prefetch=1, grid=(n_m,),
            in_specs=[pl.BlockSpec((tm, dim), spot)]
            + [pl.BlockSpec((tm, t.shape[1]), lambda m, p: (m, 0)) for t in totals]
            + [pl.BlockSpec(memory_space=pl.ANY)] * aliased,
            out_specs=pl.BlockSpec((tm, dim), spot)),
        out_shape=jax.ShapeDtypeStruct((rows, dim), BF16),
        input_output_aliases={2 + len(totals): 0} if aliased else {},
        compiler_params=params(("arbitrary",)),
        cost_estimate=cost(5e9, seq * dim * 6),
        name="residual",
    )(idx, x, *totals, *([y] if aliased else []))


def rope_tables(seq_len, head_dim):
    half = head_dim // 2
    inv_freq = 10000.0 ** (-2.0 * jnp.arange(half, dtype=F32) / head_dim)
    angles = jnp.arange(seq_len, dtype=F32)[:, None] * inv_freq[None, :]
    return jnp.cos(angles), jnp.sin(angles)


def solution(mesh):
    n_wg = mesh.shape['wg']
    batch_spec = P(('dp', 'wg'), None, None)
    in_specs = (batch_spec, P(('dp', 'wg'), None), P(None), P('wg', 'tp'), P('wg', None),
                P('wg', 'tp'), P('wg', 'tp'), P('tp', 'wg'), P('tp', 'wg'))
    out_specs = (batch_spec, batch_spec, batch_spec)
    to_right = [(i, (i + 2) % n_wg) for i in range(n_wg)]
    to_left = [(i, (i - 2) % n_wg) for i in range(n_wg)]
    far_right = [(i, (i + 4) % n_wg) for i in range(n_wg)]
    far_left = [(i, (i - 4) % n_wg) for i in range(n_wg)]
    to_pair = [(i, i ^ 1) for i in range(n_wg)]

    def shift(val, pairs):
        return lax.ppermute(val, 'wg', pairs)

    def halves(v):
        return v[:v.shape[0] // 2], v[v.shape[0] // 2:]

    def spread(shard):
        top, bottom = halves(shard)
        out = []
        for v, pairs in ((shard, to_right), (shard, to_left), (top, far_right), (bottom, far_left)):
            out.append(shift(v, pairs))
        return tuple(out)

    def swaps(vals):
        out = []
        for v in vals:
            out.append(shift(v, to_pair))
        return tuple(out)


    def ring_one(top, bottom):
        out = []
        for v, pairs in ((top, to_right), (bottom, to_left), (bottom, to_right), (top, to_left)):
            out.append(shift(v, pairs))
        return tuple(out)

    def ring_two(got):
        top = shift(got[0], to_right)
        bottom = shift(got[1], to_left)
        return top, bottom


    def local_step(x_in, valid, ln_gain, w_q, w_kv, w_gate, w_up, w_o, w_down):
        n_prompts, seq, dim = x_in.shape
        hd = w_kv.shape[1] // 2
        ff = w_gate.shape[1]
        me = lax.axis_index('wg')
        chip, core = me // 2, me % 2
        n_chip = n_wg // 2
        order = []
        for step in (0, -1, 1, 2):
            c = (chip + step + n_chip) % n_chip
            order += [2 * c + core, 2 * c + 1 - core]
        idx = jnp.stack(order).astype(jnp.int32)
        block = jnp.arange(n_wg, dtype=jnp.int32)
        away = (block // 2 - chip + n_chip) % n_chip
        slot = jnp.where(away == 0, 0, jnp.where(away == n_chip - 1, 1, jnp.where(away == 1, 2, 3)))
        pos = 2 * slot + (block % 2 != core).astype(jnp.int32)

        x2 = x_in.reshape(n_prompts * seq, dim)
        oc = w_o.shape[0]
        cut_at = 5 * FF_TILE

        def chunk(gate, up, lo, hi):
            pair = [gate[:, lo:hi], up[:, lo:hi]]
            return tuple(jnp.concatenate([halves(v)[i] for v in pair], axis=1) for i in range(2))

        def tie(vals, *deps):
            return lax.optimization_barrier(tuple(vals) + deps)[:len(vals)]

        def k_pieces(own, got):
            sw = swaps((own,) + got)
            return [own, sw[0], got[0], sw[1], got[1], sw[2], got[2], got[3], sw[3], sw[4]]

        def ring_pieces(near, sw_near, far, sw_far):
            out = []
            for i, j in ((0, 1), (2, 4), (5, 3)):
                out += [near[i], near[j], sw_near[i], sw_near[j]]
            return out + list(far) + list(sw_far)

        s_q = jnp.concatenate([w_q, w_kv], axis=1)
        got_q = spread(s_q)
        cos_t, sin_t = rope_tables(seq, hd)
        valid_col = valid.reshape(-1, 1)
        valid_row = valid.reshape(n_prompts, 1, seq)

        z0 = layer_norm(after(x2, s_q), ln_gain, pos, 0, seq)
        s_a = chunk(*tie([w_gate, w_up], z0), 0, cut_at)
        one_a = ring_one(*s_a)
        got_q = tie(got_q, *s_a)
        p_q = k_pieces(s_q, got_q)
        z1 = layer_norm(after(x2, *got_q), ln_gain, pos, 1, seq)
        s_b = chunk(*tie([w_gate, w_up], z1), cut_at, ff)
        q0, k_cache, v_cache, v0 = qkv(after(z0, *s_b), p_q, cos_t, sin_t, valid_col, hd, 0, ())
        act0 = attention(q0, k_cache, v0, valid_row, 0, oc + ff)

        near_a = tie(s_a + one_a, act0)
        far_a = ring_two(near_a[2:])
        sw_near = swaps(near_a)
        q1, k_cache, v_cache, v1 = qkv(after(z1, *near_a), p_q, cos_t, sin_t, valid_col, hd, 1,
                                          (k_cache, v_cache))
        s_b = tie(s_b, q1)
        one_b = ring_one(*s_b)
        far_a = tie(far_a, *s_b)
        p_a = ring_pieces(near_a, sw_near, far_a, swaps(far_a))
        act0 = gate_up(z0, p_a, act0, oc, 0, 3)

        near_b = tie(s_b + one_b, act0)
        far_b = ring_two(near_b[2:])
        sw_near = swaps(near_b)
        act0 = gate_up(z0, p_a, after(act0, *near_b), oc, 3, None)
        top_d, bottom_d = tie(halves(jnp.concatenate(tie([w_o, w_down], q1), axis=0)), act0)
        one_d = ring_one(top_d, bottom_d)
        far_b = tie(far_b, act0)
        p_b = ring_pieces(near_b, sw_near, far_b, swaps(far_b))
        own_d = swaps((top_d, bottom_d))
        act0 = gate_up(z0, p_b, act0, oc + cut_at)

        pair_0 = ([top_d, bottom_d], list(own_d))
        part_a = down(act0, [pair_0])
        tot_a = lax.psum(part_a, 'tp')
        one_d = tie(one_d, part_a)
        far_d = ring_two(one_d)
        sw_near = swaps(one_d)
        near = [([one_d[0], one_d[2]], [sw_near[0], sw_near[2]]), ([one_d[3], one_d[1]], [sw_near[3], sw_near[1]])]
        part_b = down(after(act0, *one_d), near, dim - part_a.shape[1])
        far_d = tie(far_d, part_b)
        sw_far = swaps(far_d)
        pair_3 = (list(far_d), list(sw_far))
        part_b = down(act0, [pair_3], dim - part_a.shape[1], 2, part_b)
        tot_b = lax.psum(after(part_b, tot_a), 'tp')

        act1 = attention(after(q1, part_b), k_cache, v1, valid_row, 1, oc + ff)
        act1 = gate_up(z1, p_a, act1, oc)
        act1 = gate_up(z1, p_b, act1, oc + cut_at)
        part_c = down(act1, [pair_0] + near + [pair_3])
        tot_c = lax.psum(after(part_c, tot_b), 'tp')

        y = residual(x2, [tot_a, tot_b], idx, None, 0, seq)
        y = residual(x2, [tot_c], idx, y, 1, seq)
        out3 = lambda v: v.reshape(n_prompts, seq, v.shape[-1])
        return out3(y), out3(k_cache), out3(v_cache)

    return jax.shard_map(local_step, mesh=mesh, in_specs=in_specs, out_specs=out_specs, check_vma=False)
```

```python
import functools

import jax
import jax.numpy as jnp
from jax import lax
from jax.experimental import pallas as pl
from jax.experimental.pallas import tpu as pltpu
from jax.sharding import PartitionSpec as P


F32 = jnp.float32
BF16 = jnp.bfloat16
N_PIECES = 8
FF_TILE = 512
CHIP_STEPS = (0, -1, 1, 2)
VMEM_LIMIT = 60 * 1024 * 1024


def after(val, *deps):
    return lax.optimization_barrier((val,) + deps)[0]


def params(sem):
    return pltpu.CompilerParams(dimension_semantics=sem, vmem_limit_bytes=VMEM_LIMIT)


def cost(flops, nbytes):
    return pl.CostEstimate(flops=int(flops), bytes_accessed=int(nbytes), transcendentals=0)


def ln_kernel(pos_ref, x_ref, gain_ref, z_ref):
    sub = 32
    blk = x_ref.shape[1] // N_PIECES

    def body(i, carry):
        rows = pl.ds(pl.multiple_of(i * sub, sub), sub)
        x = x_ref[rows, :].astype(F32)
        mean = jnp.mean(x, axis=-1, keepdims=True)
        cen = x - mean
        var = jnp.mean(cen * cen, axis=-1, keepdims=True)
        z = (cen * lax.rsqrt(var + 1e-6) * gain_ref[...]).astype(BF16)
        for j in range(N_PIECES):
            z_ref[rows, pl.ds(pl.multiple_of(pos_ref[j] * blk, blk), blk)] = z[:, j * blk:(j + 1) * blk]
        return carry

    lax.fori_loop(0, x_ref.shape[0] // sub, body, 0, unroll=2)


def layer_norm(x, gain, pos, prompt, seq):
    dim = x.shape[1]
    tm = 512
    n_m = seq // tm
    return pl.pallas_call(
        ln_kernel,
        grid_spec=pltpu.PrefetchScalarGridSpec(
            num_scalar_prefetch=1, grid=(n_m,),
            in_specs=[pl.BlockSpec((tm, dim), lambda i, p: (prompt * n_m + i, 0)),
                      pl.BlockSpec((1, dim), lambda i, p: (0, 0))],
            out_specs=pl.BlockSpec((tm, dim), lambda i, p: (i, 0))),
        out_shape=jax.ShapeDtypeStruct((seq, dim), BF16),
        compiler_params=params(("arbitrary",)),
        cost_estimate=cost(5e9, seq * dim * 4),
        name="ln",
    )(pos, x, gain.reshape(1, dim))


def fill_rows(w_s, pieces, col=0):
    row = 0
    for p in pieces:
        w_s[pl.ds(row, p.shape[0]), pl.ds(col, p.shape[1])] = p[...]
        row += p.shape[0]


def apply_rope(vals, cos_t, sin_t):
    half = vals.shape[-1] // 2
    a, b = vals[:, :half], vals[:, half:]
    return a * cos_t - b * sin_t, b * cos_t + a * sin_t


def qkv_kernel(n_heads, hd, aliased, *refs):
    z_ref, cos_ref, sin_ref, valid_ref = refs[:4]
    pieces = refs[4:-5 - aliased]
    q_ref, k_ref, v_ref, vr_ref, w_s = refs[-5:]

    @pl.when(pl.program_id(0) == 0)
    def _():
        fill_rows(w_s, pieces)

    half = hd // 2
    sub = 256
    for r in range(0, z_ref.shape[0], sub):
        rows = pl.ds(r, sub)
        out = jnp.dot(z_ref[rows, :], w_s[...], preferred_element_type=F32).astype(BF16)
        cos_t, sin_t = cos_ref[rows, :], sin_ref[rows, :]
        keep = valid_ref[rows, :] > 0
        for h in range(n_heads):
            a, b = apply_rope(out[:, h * hd:(h + 1) * hd].astype(F32), cos_t, sin_t)
            q_ref[rows, h * hd:h * hd + half] = a.astype(BF16)
            q_ref[rows, h * hd + half:(h + 1) * hd] = b.astype(BF16)
        base = n_heads * hd
        a, b = apply_rope(out[:, base:base + hd].astype(F32), cos_t, sin_t)
        k_ref[rows, :half] = jnp.where(keep, a, 0.0).astype(BF16)
        k_ref[rows, half:] = jnp.where(keep, b, 0.0).astype(BF16)
        v = out[:, base + hd:]
        vr_ref[rows, :] = v
        v_ref[rows, :] = jnp.where(keep, v.astype(F32), 0.0).astype(BF16)


def qkv(z, pieces, cos_t, sin_t, valid_col, hd, prompt, caches):
    seq, dim = z.shape
    rows = valid_col.shape[0]
    cols = pieces[0].shape[1]
    n_heads = cols // hd - 2
    tm = 1024
    n_m = seq // tm
    full = lambda p: pl.BlockSpec(p.shape, lambda i: (0, 0))
    ops = [z, cos_t, sin_t, valid_col] + list(pieces) + list(caches)
    at = len(ops) - len(caches)
    cache_spec = pl.BlockSpec((tm, hd), lambda i: (prompt * n_m + i, 0))
    return pl.pallas_call(
        functools.partial(qkv_kernel, n_heads, hd, len(caches)),
        grid=(n_m,),
        in_specs=[pl.BlockSpec((tm, dim), lambda i: (i, 0)),
                  pl.BlockSpec((tm, hd // 2), lambda i: (i, 0)),
                  pl.BlockSpec((tm, hd // 2), lambda i: (i, 0)),
                  pl.BlockSpec((tm, 1), lambda i: (prompt * n_m + i, 0))] + [full(p) for p in pieces]
        + [pl.BlockSpec(memory_space=pl.ANY)] * len(caches),
        out_specs=[pl.BlockSpec((tm, n_heads * hd), lambda i: (i, 0)), cache_spec, cache_spec,
                   pl.BlockSpec((tm, hd), lambda i: (i, 0))],
        out_shape=[jax.ShapeDtypeStruct((seq, n_heads * hd), BF16)] + [jax.ShapeDtypeStruct((rows, hd), BF16)] * 2
        + [jax.ShapeDtypeStruct((seq, hd), BF16)],
        scratch_shapes=[pltpu.VMEM((dim, cols), BF16)],
        input_output_aliases={at + i: 1 + i for i in range(len(caches))},
        compiler_params=params(("arbitrary",)),
        cost_estimate=cost(2 * seq * dim * cols, seq * dim * 4),
        name="qkv",
    )(*ops)


def attn_kernel(n_blk, scale, hd, q_ref, k_ref, v_ref, valid_ref, o_ref):
    i = pl.program_id(0)
    blk = q_ref.shape[0]
    dn = (((1,), (1,)), ((), ()))

    def block(b):
        past = b * blk
        rows = lax.broadcasted_iota(jnp.int32, (blk, blk), 0)
        cols = lax.broadcasted_iota(jnp.int32, (blk, blk), 1)
        ok1 = jnp.logical_and(cols <= rows, valid_ref[:, past:past + blk] > 0)
        for h in range(q_ref.shape[1] // hd):
            q = q_ref[:, h * hd:(h + 1) * hd]
            s1 = lax.dot_general(q, k_ref[past:past + blk, :], dn, preferred_element_type=F32) * scale
            s1 = jnp.where(ok1, s1, -1e30)
            top = jnp.max(s1, axis=-1, keepdims=True)
            if b:
                s0 = lax.dot_general(q, k_ref[:past, :], dn, preferred_element_type=F32) * scale
                s0 = jnp.where(valid_ref[:, :past] > 0, s0, -1e30)
                top = jnp.maximum(top, jnp.max(s0, axis=-1, keepdims=True))
                e0 = jnp.exp(s0 - top)
            e1 = jnp.exp(s1 - top)
            tot = jnp.sum(e1, axis=-1, keepdims=True)
            if b:
                tot = tot + jnp.sum(e0, axis=-1, keepdims=True)
            inv = 1.0 / tot
            out = jnp.dot((e1 * inv).astype(BF16), v_ref[past:past + blk, :], preferred_element_type=F32)
            if b:
                out = out + jnp.dot((e0 * inv).astype(BF16), v_ref[:past, :], preferred_element_type=F32)
            o_ref[:, h * hd:(h + 1) * hd] = out.astype(BF16)

    for b in range(n_blk):
        pl.when(i == b)(functools.partial(block, b))


def attention(q, k, v, valid_row, prompt, act_cols):
    seq, hd = v.shape
    q_cols = q.shape[1]
    blk = 512
    n_blk = seq // blk
    return pl.pallas_call(
        functools.partial(attn_kernel, n_blk, hd ** -0.5, hd),
        grid=(n_blk,),
        in_specs=[pl.BlockSpec((blk, q_cols), lambda i: (i, 0)),
                  pl.BlockSpec((seq, hd), lambda i: (prompt, 0)),
                  pl.BlockSpec((seq, hd), lambda i: (0, 0)),
                  pl.BlockSpec((None, 1, seq), lambda i: (prompt, 0, 0))],
        out_specs=pl.BlockSpec((blk, q_cols), lambda i: (i, 0)),
        out_shape=jax.ShapeDtypeStruct((seq, act_cols), BF16),
        compiler_params=params(("arbitrary",)),
        cost_estimate=cost(16e9, seq * hd * 12),
        name="attn",
    )(q, k, v, valid_row)


def gu_kernel(*refs):
    z_ref = refs[0]
    pieces = refs[1:-3]
    m_ref, w_s = refs[-2:]

    @pl.when(pl.program_id(1) == 0)
    def _():
        fill_rows(w_s, pieces[:len(pieces) // 2])
        fill_rows(w_s, pieces[len(pieces) // 2:], w_s.shape[1] // 2)

    t = m_ref.shape[1]
    sub = 256
    for r in range(0, z_ref.shape[0], sub):
        rows = pl.ds(r, sub)
        out = jnp.dot(z_ref[rows, :], w_s[...], preferred_element_type=F32).astype(BF16)
        a = out[:, :t].astype(F32)
        u = out[:, t:].astype(F32)
        m_ref[rows, :] = (a * jax.nn.sigmoid(a) * u).astype(BF16)


def gate_up(z, pieces, act, first_col, lo=0, hi=None):
    seq, dim = z.shape
    n_tiles = pieces[0].shape[1] // (2 * FF_TILE)
    hi = n_tiles if hi is None else hi
    cols = (hi - lo) * 2 * FF_TILE
    tm = 1024
    first = first_col // FF_TILE + lo
    ops = [z] + list(pieces) + list(pieces) + [act]
    return pl.pallas_call(
        gu_kernel,
        grid=(cols // (2 * FF_TILE), seq // tm),
        in_specs=[pl.BlockSpec((tm, dim), lambda n, m: (m, 0))]
        + [pl.BlockSpec((p.shape[0], FF_TILE), lambda n, m: (0, lo + n)) for p in pieces]
        + [pl.BlockSpec((p.shape[0], FF_TILE), lambda n, m: (0, n_tiles + lo + n)) for p in pieces]
        + [pl.BlockSpec(memory_space=pl.ANY)],
        out_specs=pl.BlockSpec((tm, FF_TILE), lambda n, m: (m, first + n)),
        out_shape=jax.ShapeDtypeStruct(act.shape, BF16),
        scratch_shapes=[pltpu.VMEM((dim, 2 * FF_TILE), BF16)],
        input_output_aliases={len(ops) - 1: 0},
        compiler_params=params(("arbitrary", "arbitrary")),
        cost_estimate=cost(2 * seq * dim * cols, seq * dim * 4),
        name="gate_up",
    )(*ops)


def down_kernel(plan, act_ref, *refs):
    n_w = sum(len(p) for p in plan)
    w_refs = refs[:n_w]
    out_ref, w_s, sems = refs[-3:]
    j, m = pl.program_id(0), pl.program_id(1)

    def copies(t):
        at = sum(len(p) for p in plan[:t])
        slot = t % 2
        return [pltpu.make_async_copy(w_refs[at + i], w_s.at[slot, pl.ds(row, w_refs[at + i].shape[0]), pl.ds(col, w_refs[at + i].shape[1])],
                                      sems.at[slot, i]) for i, (row, col) in enumerate(plan[t])]

    for t in range(len(plan)):
        @pl.when(jnp.logical_and(j == t, m == 0))
        def _(t=t):
            if t == 0:
                for c in copies(0):
                    c.start()
            for c in copies(t):
                c.wait()
            if t + 1 < len(plan):
                for c in copies(t + 1):
                    c.start()

    slot = lax.rem(j, 2)
    sub = 256
    for r in range(0, out_ref.shape[0], sub):
        rows = pl.ds(r, sub)
        out_ref[rows, :] = jnp.dot(act_ref[rows, :], w_s[slot], preferred_element_type=F32).astype(BF16)


def down(act, pairs, n_cols=None, first=0, buf=None):
    seq, kdim = act.shape
    blk = pairs[0][0][0].shape[1]
    tm = 512
    plan, ws = [], []
    for pair in pairs:
        spots = []
        for side, group in enumerate(pair):
            row = 0
            for p in group:
                spots.append((row, side * blk))
                ws.append(p)
                row += p.shape[0]
        plan.append(spots)
    n_cols = n_cols or 2 * blk * len(pairs)
    aliased = 0 if buf is None else 1
    ops = [act] + ws + ([buf] if aliased else [])
    return pl.pallas_call(
        functools.partial(down_kernel, plan),
        grid=(len(pairs), seq // tm),
        in_specs=[pl.BlockSpec((tm, kdim), lambda j, m: (m, 0))] + [pl.BlockSpec(memory_space=pl.ANY)] * (len(ws) + aliased),
        out_specs=pl.BlockSpec((tm, 2 * blk), lambda j, m: (m, first + j)),
        out_shape=jax.ShapeDtypeStruct((seq, n_cols), BF16),
        scratch_shapes=[pltpu.VMEM((2, kdim, 2 * blk), BF16), pltpu.SemaphoreType.DMA((2, 4))],
        input_output_aliases={len(ops) - 1: 0} if aliased else {},
        compiler_params=params(("arbitrary", "arbitrary")),
        cost_estimate=cost(2 * seq * kdim * 2 * blk * len(pairs), seq * kdim * 2),
        name="down",
    )(*ops)


def ring_kernel(n_w, *refs):
    act_ref, x_ref, w_refs, y_ref = refs[0], refs[1], refs[2:2 + n_w], refs[2 + n_w]
    act_s, w_s, part, got, total, act_sem, w_sem, send_sem, recv_sem, out_sem = refs[3 + n_w:]
    dim = x_ref.shape[1]
    chip, core = lax.axis_index("wg") // 2, lax.axis_index("wg") % 2
    n_chip = lax.axis_size("wg") // 2
    n_pairs, _, seq, blk = part.shape
    n_tp = lax.axis_size("tp")
    d = lax.axis_index("tp")
    quarter = seq // n_tp
    n_steps = 2 * (n_tp - 1)
    half_rows = act_s.shape[1]
    per = n_w // n_pairs
    k_half = w_refs[0].shape[0]

    barrier = pltpu.get_barrier_semaphore()
    for sg in (1, -1):
        pl.semaphore_signal(barrier, inc=1, device_id={"tp": lax.rem(d + sg + n_tp, n_tp)},
                            device_id_type=pl.DeviceIdType.MESH)
    pl.semaphore_wait(barrier, 2)

    def act_copy(i):
        return pltpu.make_async_copy(act_ref.at[pl.ds(i * half_rows, half_rows), :], act_s.at[i], act_sem.at[i])

    def w_copies(t):
        out = []
        for i in range(per):
            side, row = i // 2, (i % 2) * k_half
            dst = w_s.at[t % 2, pl.ds(row, k_half), pl.ds(side * blk, blk)]
            out.append(pltpu.make_async_copy(w_refs[t * per + i], dst, w_sem.at[t % 2, i]))
        return out

    def rows_of(q):
        return pl.ds(pl.multiple_of(lax.rem(q + 2 * n_tp, n_tp) * quarter, quarter), quarter)

    def ring_copy(t, side, s):
        sg = 1 - 2 * side
        if s < n_tp - 1:
            src, dst = part.at[t, side, rows_of(d - sg * s), :], got.at[t, side, s]
        else:
            rows = rows_of(d + sg * (n_tp - s))
            src, dst = total.at[t, side, rows, :], total.at[t, side, rows, :]
        return pltpu.make_async_remote_copy(
            src_ref=src, dst_ref=dst, send_sem=send_sem.at[t, side, s], recv_sem=recv_sem.at[t, side, s],
            device_id={"tp": lax.rem(d + sg + n_tp, n_tp)}, device_id_type=pl.DeviceIdType.MESH)

    def x_copy(i, first):
        return pltpu.make_async_copy(x_ref.at[pl.ds(first + i * half_rows, half_rows), :],
                                     act_s.at[i, :, pl.ds(0, dim)], act_sem.at[i])

    def place(t, side, k):
        q = lax.rem(d + (1 - 2 * side) * (1 - k) + 2 * n_tp, n_tp)
        here = lax.rem(chip + CHIP_STEPS[t] + n_chip, n_chip) * 2 + (core if side == 0 else 1 - core)
        per_half = half_rows // quarter
        return q, q // per_half, (q % per_half) * quarter, pl.multiple_of(here * blk, blk)

    def out_copy(t, side, k):
        q, h, row, col = place(t, side, k)
        src = act_s.at[h, pl.ds(pl.multiple_of(row, quarter), quarter), pl.ds(col, blk)]
        dst = y_ref.at[pl.ds(pl.multiple_of(y_ref.shape[0] - seq + q * quarter, quarter), quarter), pl.ds(col, blk)]
        return pltpu.make_async_copy(src, dst, out_sem.at[t, side, k])

    def finish(t, side, k):
        q, h, row, col = place(t, side, k)

        def add(i, carry):
            at = i * 128
            spot = (h, pl.ds(pl.multiple_of(row + at, 128), 128), pl.ds(col, blk))
            tot = total[t, side, pl.ds(pl.multiple_of(q * quarter + at, 128), 128), :]
            act_s[spot] = (act_s[spot].astype(F32) + tot.astype(F32)).astype(BF16)
            return carry

        lax.fori_loop(0, quarter // 128, add, 0)

    def action(t, s):
        for side in range(2):
            sg = 1 - 2 * side
            if s:
                ring_copy(t, side, s - 1).wait_recv()
            if 0 < s < n_tp:
                q = lax.rem(d - sg * s + 2 * n_tp, n_tp) * quarter
                into = part if s < n_tp - 1 else total

                def add(i, carry, side=side, q=q, into=into):
                    at = pl.multiple_of(i * 128, 128)
                    rows = pl.ds(pl.multiple_of(q + at, 128), 128)
                    into[t, side, rows, :] = (part[t, side, rows, :].astype(F32)
                                              + got[t, side, s - 1, pl.ds(at, 128), :].astype(F32)).astype(BF16)
                    return carry

                lax.fori_loop(0, quarter // 128, add, 0)
        for side in range(2):
            if s < n_steps:
                ring_copy(t, side, s).start()
        if s >= n_tp - 1:
            for side in range(2):
                finish(t, side, s - (n_tp - 1))
            for side in range(2):
                out_copy(t, side, s - (n_tp - 1)).start()

    for i in range(2):
        act_copy(i).start()
    for c in w_copies(0):
        c.start()

    def pair(t, carry):
        for tt in range(n_pairs):
            @pl.when(t == tt)
            def _(tt=tt):
                for c in w_copies(tt):
                    c.wait()
                if tt + 1 < n_pairs:
                    for c in w_copies(tt + 1):
                        c.start()
        for i in range(2):
            @pl.when(t == 0)
            def _(i=i):
                act_copy(i).wait()

            def tile(r, c2, i=i):
                at = pl.multiple_of(r * 256, 256)
                out = jnp.dot(act_s[i, pl.ds(at, 256), :], w_s[lax.rem(t, 2)], preferred_element_type=F32).astype(BF16)
                rows = pl.ds(pl.multiple_of(i * half_rows + at, 256), 256)
                part[t, 0, rows, :] = out[:, :blk]
                part[t, 1, rows, :] = out[:, blk:]
                return c2

            lax.fori_loop(0, half_rows // 256, tile, 0)

            @pl.when(t > 0)
            def _(i=i):
                action(t - 1, 1 + i)
        action(t, 0)
        return carry

    lax.fori_loop(0, n_pairs, pair, 0)
    for i in range(2):
        x_copy(i, y_ref.shape[0] - seq).start()
    for i in range(2):
        x_copy(i, y_ref.shape[0] - seq).wait()

    state = [3] * (n_pairs - 1) + [1]
    while min(state) <= n_steps:
        for t in [n_pairs - 1] + list(range(n_pairs - 1)):
            if state[t] <= n_steps and (t == n_pairs - 1 or state[t] <= state[-1] + 1):
                action(t, state[t])
                state[t] += 1

    for t in range(n_pairs):
        for side in range(2):
            for s in range(n_steps):
                ring_copy(t, side, s).wait_send()
            for k in range(n_tp):
                out_copy(t, side, k).wait()


def down_ring(act, x, pairs):
    seq, kdim = act.shape
    ws = [p for pair in pairs for group in pair for p in group]
    blk = ws[0].shape[1]
    n_pairs = len(pairs)
    n_tp = lax.axis_size("tp")
    n_steps = 2 * (n_tp - 1)
    shape = (n_pairs, 2, seq, blk)
    return pl.pallas_call(
        functools.partial(ring_kernel, len(ws)),
        in_specs=[pl.BlockSpec(memory_space=pl.ANY)] * (2 + len(ws)),
        out_specs=pl.BlockSpec(memory_space=pl.ANY),
        out_shape=jax.ShapeDtypeStruct(x.shape, BF16),
        scratch_shapes=[pltpu.VMEM((2, seq // 2, kdim), BF16), pltpu.VMEM((2, kdim, 2 * blk), BF16),
                        pltpu.VMEM(shape, BF16), pltpu.VMEM((n_pairs, 2, n_tp - 1, seq // n_tp, blk), BF16),
                        pltpu.VMEM(shape, BF16),
                        pltpu.SemaphoreType.DMA((2,)), pltpu.SemaphoreType.DMA((2, len(ws) // n_pairs)),
                        pltpu.SemaphoreType.DMA((n_pairs, 2, n_steps)), pltpu.SemaphoreType.DMA((n_pairs, 2, n_steps)),
                        pltpu.SemaphoreType.DMA((n_pairs, 2, n_tp))],
        compiler_params=pltpu.CompilerParams(collective_id=0, has_side_effects=True, vmem_limit_bytes=VMEM_LIMIT),
        cost_estimate=cost(1.4e11, seq * kdim * 2),
        name="down_ring",
    )(act, x, *ws)


def add_kernel(n_tot, idx_ref, x_ref, *refs):
    tots, y_ref = refs[:n_tot], refs[-1]
    blk = x_ref.shape[1] // N_PIECES
    j = 0
    for t in tots:
        if len(t.shape) == 4:
            parts = [t[i, side] for i in range(t.shape[0]) for side in range(2)]
        else:
            parts = [t[:, c:c + blk] for c in range(0, t.shape[1], blk)]
        for v in parts:
            spot = pl.ds(pl.multiple_of(idx_ref[j] * blk, blk), blk)
            y_ref[:, spot] = (x_ref[:, spot].astype(F32) + v.astype(F32)).astype(BF16)
            j += 1


def residual(x, totals, idx, y, prompt, seq):
    rows, dim = x.shape
    tm = 512
    n_m = seq // tm
    aliased = 0 if y is None else 1
    spot = lambda m, p: (prompt * n_m + m, 0)
    return pl.pallas_call(
        functools.partial(add_kernel, len(totals)),
        grid_spec=pltpu.PrefetchScalarGridSpec(
            num_scalar_prefetch=1, grid=(n_m,),
            in_specs=[pl.BlockSpec((tm, dim), spot)]
            + [pl.BlockSpec((tm, t.shape[1]), lambda m, p: (m, 0)) if t.ndim == 2 else
               pl.BlockSpec(t.shape[:2] + (tm, t.shape[3]), lambda m, p: (0, 0, m, 0)) for t in totals]
            + [pl.BlockSpec(memory_space=pl.ANY)] * aliased,
            out_specs=pl.BlockSpec((tm, dim), spot)),
        out_shape=jax.ShapeDtypeStruct((rows, dim), BF16),
        input_output_aliases={2 + len(totals): 0} if aliased else {},
        compiler_params=params(("arbitrary",)),
        cost_estimate=cost(5e9, seq * dim * 6),
        name="residual",
    )(idx, x, *totals, *([y] if aliased else []))


def rope_tables(seq_len, head_dim):
    half = head_dim // 2
    inv_freq = 10000.0 ** (-2.0 * jnp.arange(half, dtype=F32) / head_dim)
    angles = jnp.arange(seq_len, dtype=F32)[:, None] * inv_freq[None, :]
    return jnp.cos(angles), jnp.sin(angles)


def solution(mesh):
    n_wg = mesh.shape['wg']
    batch_spec = P(('dp', 'wg'), None, None)
    in_specs = (batch_spec, P(('dp', 'wg'), None), P(None), P('wg', 'tp'), P('wg', None),
                P('wg', 'tp'), P('wg', 'tp'), P('tp', 'wg'), P('tp', 'wg'))
    out_specs = (batch_spec, batch_spec, batch_spec)
    to_right = [(i, (i + 2) % n_wg) for i in range(n_wg)]
    to_left = [(i, (i - 2) % n_wg) for i in range(n_wg)]
    far_right = [(i, (i + 4) % n_wg) for i in range(n_wg)]
    far_left = [(i, (i - 4) % n_wg) for i in range(n_wg)]
    to_pair = [(i, i ^ 1) for i in range(n_wg)]

    def shift(val, pairs):
        return lax.ppermute(val, 'wg', pairs)

    def halves(v):
        return v[:v.shape[0] // 2], v[v.shape[0] // 2:]

    def spread(shard):
        top, bottom = halves(shard)
        out = []
        for v, pairs in ((shard, to_right), (shard, to_left), (top, far_right), (bottom, far_left)):
            out.append(shift(v, pairs))
        return tuple(out)

    def swaps(vals):
        out = []
        for v in vals:
            out.append(shift(v, to_pair))
        return tuple(out)


    def ring_one(top, bottom):
        out = []
        for v, pairs in ((top, to_right), (bottom, to_left), (bottom, to_right), (top, to_left)):
            out.append(shift(v, pairs))
        return tuple(out)

    def ring_two(got):
        top = shift(got[0], to_right)
        bottom = shift(got[1], to_left)
        return top, bottom


    def local_step(x_in, valid, ln_gain, w_q, w_kv, w_gate, w_up, w_o, w_down):
        n_prompts, seq, dim = x_in.shape
        hd = w_kv.shape[1] // 2
        ff = w_gate.shape[1]
        me = lax.axis_index('wg')
        chip, core = me // 2, me % 2
        n_chip = n_wg // 2
        order = []
        for step in CHIP_STEPS:
            c = (chip + step + n_chip) % n_chip
            order += [2 * c + core, 2 * c + 1 - core]
        idx = jnp.stack(order).astype(jnp.int32)
        block = jnp.arange(n_wg, dtype=jnp.int32)
        away = (block // 2 - chip + n_chip) % n_chip
        slot = jnp.where(away == 0, 0, jnp.where(away == n_chip - 1, 1, jnp.where(away == 1, 2, 3)))
        pos = 2 * slot + (block % 2 != core).astype(jnp.int32)

        x2 = x_in.reshape(n_prompts * seq, dim)
        oc = w_o.shape[0]
        cut_at = 5 * FF_TILE

        def chunk(gate, up, lo, hi):
            pair = [gate[:, lo:hi], up[:, lo:hi]]
            return tuple(jnp.concatenate([halves(v)[i] for v in pair], axis=1) for i in range(2))

        def tie(vals, *deps):
            return lax.optimization_barrier(tuple(vals) + deps)[:len(vals)]

        def k_pieces(own, got):
            sw = swaps((own,) + got)
            return [own, sw[0], got[0], sw[1], got[1], sw[2], got[2], got[3], sw[3], sw[4]]

        def ring_pieces(near, sw_near, far, sw_far):
            out = []
            for i, j in ((0, 1), (2, 4), (5, 3)):
                out += [near[i], near[j], sw_near[i], sw_near[j]]
            return out + list(far) + list(sw_far)

        s_q = jnp.concatenate([w_q, w_kv], axis=1)
        got_q = spread(s_q)
        cos_t, sin_t = rope_tables(seq, hd)
        valid_col = valid.reshape(-1, 1)
        valid_row = valid.reshape(n_prompts, 1, seq)

        z0 = layer_norm(after(x2, s_q), ln_gain, pos, 0, seq)
        s_a = chunk(*tie([w_gate, w_up], z0), 0, cut_at)
        one_a = ring_one(*s_a)
        got_q = tie(got_q, *s_a)
        p_q = k_pieces(s_q, got_q)
        z1 = layer_norm(after(x2, *got_q), ln_gain, pos, 1, seq)
        s_b = chunk(*tie([w_gate, w_up], z1), cut_at, ff)
        q0, k_cache, v_cache, v0 = qkv(after(z0, *s_b), p_q, cos_t, sin_t, valid_col, hd, 0, ())
        act0 = attention(q0, k_cache, v0, valid_row, 0, oc + ff)

        near_a = tie(s_a + one_a, act0)
        far_a = ring_two(near_a[2:])
        sw_near = swaps(near_a)
        q1, k_cache, v_cache, v1 = qkv(after(z1, *near_a), p_q, cos_t, sin_t, valid_col, hd, 1,
                                          (k_cache, v_cache))
        s_b = tie(s_b, q1)
        one_b = ring_one(*s_b)
        act1 = attention(after(q1, *s_b), k_cache, v1, valid_row, 1, oc + ff)
        far_a = tie(far_a, act1)
        p_a = ring_pieces(near_a, sw_near, far_a, swaps(far_a))
        act0 = gate_up(z0, p_a, act0, oc, 0, 3)

        near_b = tie(s_b + one_b, act0)
        far_b = ring_two(near_b[2:])
        sw_near = swaps(near_b)
        act0 = gate_up(z0, p_a, after(act0, *near_b), oc, 3, None)
        top_d, bottom_d = tie(halves(jnp.concatenate(tie([w_o, w_down], q1), axis=0)), act0)
        one_d = ring_one(top_d, bottom_d)
        far_b = tie(far_b, act0)
        p_b = ring_pieces(near_b, sw_near, far_b, swaps(far_b))
        own_d = swaps((top_d, bottom_d))
        act0 = gate_up(z0, p_b, act0, oc + cut_at)

        pair_0 = ([top_d, bottom_d], list(own_d))
        part_a = down(act0, [pair_0])
        tot_a = lax.psum(part_a, 'tp')
        one_d = tie(one_d, part_a)
        far_d = ring_two(one_d)
        sw_near = swaps(one_d)
        near = [([one_d[0], one_d[2]], [sw_near[0], sw_near[2]]), ([one_d[3], one_d[1]], [sw_near[3], sw_near[1]])]
        part_b = down(after(act0, *one_d), near, dim - part_a.shape[1])
        far_d = tie(far_d, part_b)
        sw_far = swaps(far_d)
        pair_3 = (list(far_d), list(sw_far))
        part_b = down(act0, [pair_3], dim - part_a.shape[1], 2, part_b)
        tot_b = lax.psum(after(part_b, tot_a), 'tp')

        act1 = gate_up(z1, p_a, after(act1, part_b), oc)
        act1 = gate_up(z1, p_b, act1, oc + cut_at)
        y = down_ring(act1, x2, [pair_0] + near + [pair_3])

        y = residual(x2, [tot_a, tot_b], idx, y, 0, seq)
        out3 = lambda v: v.reshape(n_prompts, seq, v.shape[-1])
        return out3(y), out3(k_cache), out3(v_cache)

    return jax.shard_map(local_step, mesh=mesh, in_specs=in_specs, out_specs=out_specs, check_vma=False)
```

```python
import functools

import jax
import jax.numpy as jnp
from jax import lax
from jax.experimental import pallas as pl
from jax.experimental.pallas import tpu as pltpu
from jax.sharding import PartitionSpec as P


F32 = jnp.float32
BF16 = jnp.bfloat16
N_PIECES = 8
FF_TILE = 512
CHIP_STEPS = (0, -1, 1, 2)
VMEM_LIMIT = 60 * 1024 * 1024


def after(val, *deps):
    return lax.optimization_barrier((val,) + deps)[0]


def params(sem):
    return pltpu.CompilerParams(dimension_semantics=sem, vmem_limit_bytes=VMEM_LIMIT)


def cost(flops, nbytes):
    return pl.CostEstimate(flops=int(flops), bytes_accessed=int(nbytes), transcendentals=0)


def ln_kernel(pos_ref, x_ref, gain_ref, z_ref):
    sub = 32
    blk = x_ref.shape[1] // N_PIECES

    def body(i, carry):
        rows = pl.ds(pl.multiple_of(i * sub, sub), sub)
        x = x_ref[rows, :].astype(F32)
        mean = jnp.mean(x, axis=-1, keepdims=True)
        cen = x - mean
        var = jnp.mean(cen * cen, axis=-1, keepdims=True)
        z = (cen * lax.rsqrt(var + 1e-6) * gain_ref[...]).astype(BF16)
        for j in range(N_PIECES):
            z_ref[rows, pl.ds(pl.multiple_of(pos_ref[j] * blk, blk), blk)] = z[:, j * blk:(j + 1) * blk]
        return carry

    lax.fori_loop(0, x_ref.shape[0] // sub, body, 0, unroll=2)


def layer_norm(x, gain, pos, prompt, seq):
    dim = x.shape[1]
    tm = 512
    n_m = seq // tm
    return pl.pallas_call(
        ln_kernel,
        grid_spec=pltpu.PrefetchScalarGridSpec(
            num_scalar_prefetch=1, grid=(n_m,),
            in_specs=[pl.BlockSpec((tm, dim), lambda i, p: (prompt * n_m + i, 0)),
                      pl.BlockSpec((1, dim), lambda i, p: (0, 0))],
            out_specs=pl.BlockSpec((tm, dim), lambda i, p: (i, 0))),
        out_shape=jax.ShapeDtypeStruct((seq, dim), BF16),
        compiler_params=params(("arbitrary",)),
        cost_estimate=cost(5e9, seq * dim * 4),
        name="ln",
    )(pos, x, gain.reshape(1, dim))


def fill_rows(w_s, pieces, col=0):
    row = 0
    for p in pieces:
        w_s[pl.ds(row, p.shape[0]), pl.ds(col, p.shape[1])] = p[...]
        row += p.shape[0]


def apply_rope(vals, cos_t, sin_t):
    half = vals.shape[-1] // 2
    a, b = vals[:, :half], vals[:, half:]
    return a * cos_t - b * sin_t, b * cos_t + a * sin_t


def qkv_kernel(n_heads, hd, aliased, *refs):
    z_ref, cos_ref, sin_ref, valid_ref = refs[:4]
    pieces = refs[4:-5 - aliased]
    q_ref, k_ref, v_ref, vr_ref, w_s = refs[-5:]

    @pl.when(pl.program_id(0) == 0)
    def _():
        fill_rows(w_s, pieces)

    half = hd // 2
    sub = 256
    for r in range(0, z_ref.shape[0], sub):
        rows = pl.ds(r, sub)
        out = jnp.dot(z_ref[rows, :], w_s[...], preferred_element_type=F32).astype(BF16)
        cos_t, sin_t = cos_ref[rows, :], sin_ref[rows, :]
        keep = valid_ref[rows, :] > 0
        for h in range(n_heads):
            a, b = apply_rope(out[:, h * hd:(h + 1) * hd].astype(F32), cos_t, sin_t)
            q_ref[rows, h * hd:h * hd + half] = a.astype(BF16)
            q_ref[rows, h * hd + half:(h + 1) * hd] = b.astype(BF16)
        base = n_heads * hd
        a, b = apply_rope(out[:, base:base + hd].astype(F32), cos_t, sin_t)
        k_ref[rows, :half] = jnp.where(keep, a, 0.0).astype(BF16)
        k_ref[rows, half:] = jnp.where(keep, b, 0.0).astype(BF16)
        v = out[:, base + hd:]
        vr_ref[rows, :] = v
        v_ref[rows, :] = jnp.where(keep, v.astype(F32), 0.0).astype(BF16)


def qkv(z, pieces, cos_t, sin_t, valid_col, hd, prompt, caches):
    seq, dim = z.shape
    rows = valid_col.shape[0]
    cols = pieces[0].shape[1]
    n_heads = cols // hd - 2
    tm = 1024
    n_m = seq // tm
    full = lambda p: pl.BlockSpec(p.shape, lambda i: (0, 0))
    ops = [z, cos_t, sin_t, valid_col] + list(pieces) + list(caches)
    at = len(ops) - len(caches)
    cache_spec = pl.BlockSpec((tm, hd), lambda i: (prompt * n_m + i, 0))
    return pl.pallas_call(
        functools.partial(qkv_kernel, n_heads, hd, len(caches)),
        grid=(n_m,),
        in_specs=[pl.BlockSpec((tm, dim), lambda i: (i, 0)),
                  pl.BlockSpec((tm, hd // 2), lambda i: (i, 0)),
                  pl.BlockSpec((tm, hd // 2), lambda i: (i, 0)),
                  pl.BlockSpec((tm, 1), lambda i: (prompt * n_m + i, 0))] + [full(p) for p in pieces]
        + [pl.BlockSpec(memory_space=pl.ANY)] * len(caches),
        out_specs=[pl.BlockSpec((tm, n_heads * hd), lambda i: (i, 0)), cache_spec, cache_spec,
                   pl.BlockSpec((tm, hd), lambda i: (i, 0))],
        out_shape=[jax.ShapeDtypeStruct((seq, n_heads * hd), BF16)] + [jax.ShapeDtypeStruct((rows, hd), BF16)] * 2
        + [jax.ShapeDtypeStruct((seq, hd), BF16)],
        scratch_shapes=[pltpu.VMEM((dim, cols), BF16)],
        input_output_aliases={at + i: 1 + i for i in range(len(caches))},
        compiler_params=params(("arbitrary",)),
        cost_estimate=cost(2 * seq * dim * cols, seq * dim * 4),
        name="qkv",
    )(*ops)


def attn_kernel(n_blk, scale, hd, q_ref, k_ref, v_ref, valid_ref, o_ref):
    i = pl.program_id(0)
    blk = q_ref.shape[0]
    dn = (((1,), (1,)), ((), ()))

    def block(b):
        past = b * blk
        rows = lax.broadcasted_iota(jnp.int32, (blk, blk), 0)
        cols = lax.broadcasted_iota(jnp.int32, (blk, blk), 1)
        ok1 = jnp.logical_and(cols <= rows, valid_ref[:, past:past + blk] > 0)
        for h in range(q_ref.shape[1] // hd):
            q = q_ref[:, h * hd:(h + 1) * hd]
            s1 = lax.dot_general(q, k_ref[past:past + blk, :], dn, preferred_element_type=F32) * scale
            s1 = jnp.where(ok1, s1, -1e30)
            top = jnp.max(s1, axis=-1, keepdims=True)
            if b:
                s0 = lax.dot_general(q, k_ref[:past, :], dn, preferred_element_type=F32) * scale
                s0 = jnp.where(valid_ref[:, :past] > 0, s0, -1e30)
                top = jnp.maximum(top, jnp.max(s0, axis=-1, keepdims=True))
                e0 = jnp.exp(s0 - top)
            e1 = jnp.exp(s1 - top)
            tot = jnp.sum(e1, axis=-1, keepdims=True)
            if b:
                tot = tot + jnp.sum(e0, axis=-1, keepdims=True)
            inv = 1.0 / tot
            out = jnp.dot((e1 * inv).astype(BF16), v_ref[past:past + blk, :], preferred_element_type=F32)
            if b:
                out = out + jnp.dot((e0 * inv).astype(BF16), v_ref[:past, :], preferred_element_type=F32)
            o_ref[:, h * hd:(h + 1) * hd] = out.astype(BF16)

    for b in range(n_blk):
        pl.when(i == b)(functools.partial(block, b))


def attention(q, k, v, valid_row, prompt, act_cols):
    seq, hd = v.shape
    q_cols = q.shape[1]
    blk = 512
    n_blk = seq // blk
    return pl.pallas_call(
        functools.partial(attn_kernel, n_blk, hd ** -0.5, hd),
        grid=(n_blk,),
        in_specs=[pl.BlockSpec((blk, q_cols), lambda i: (i, 0)),
                  pl.BlockSpec((seq, hd), lambda i: (prompt, 0)),
                  pl.BlockSpec((seq, hd), lambda i: (0, 0)),
                  pl.BlockSpec((None, 1, seq), lambda i: (prompt, 0, 0))],
        out_specs=pl.BlockSpec((blk, q_cols), lambda i: (i, 0)),
        out_shape=jax.ShapeDtypeStruct((seq, act_cols), BF16),
        compiler_params=params(("arbitrary",)),
        cost_estimate=cost(16e9, seq * hd * 12),
        name="attn",
    )(q, k, v, valid_row)


def gu_kernel(*refs):
    z_ref = refs[0]
    pieces = refs[1:-3]
    m_ref, w_s = refs[-2:]

    @pl.when(pl.program_id(1) == 0)
    def _():
        fill_rows(w_s, pieces[:len(pieces) // 2])
        fill_rows(w_s, pieces[len(pieces) // 2:], w_s.shape[1] // 2)

    t = m_ref.shape[1]
    sub = 256
    for r in range(0, z_ref.shape[0], sub):
        rows = pl.ds(r, sub)
        out = jnp.dot(z_ref[rows, :], w_s[...], preferred_element_type=F32).astype(BF16)
        a = out[:, :t].astype(F32)
        u = out[:, t:].astype(F32)
        m_ref[rows, :] = (a * jax.nn.sigmoid(a) * u).astype(BF16)


def gate_up(z, pieces, act, first_col, lo=0, hi=None):
    seq, dim = z.shape
    n_tiles = pieces[0].shape[1] // (2 * FF_TILE)
    hi = n_tiles if hi is None else hi
    cols = (hi - lo) * 2 * FF_TILE
    tm = 1024
    first = first_col // FF_TILE + lo
    ops = [z] + list(pieces) + list(pieces) + [act]
    return pl.pallas_call(
        gu_kernel,
        grid=(cols // (2 * FF_TILE), seq // tm),
        in_specs=[pl.BlockSpec((tm, dim), lambda n, m: (m, 0))]
        + [pl.BlockSpec((p.shape[0], FF_TILE), lambda n, m: (0, lo + n)) for p in pieces]
        + [pl.BlockSpec((p.shape[0], FF_TILE), lambda n, m: (0, n_tiles + lo + n)) for p in pieces]
        + [pl.BlockSpec(memory_space=pl.ANY)],
        out_specs=pl.BlockSpec((tm, FF_TILE), lambda n, m: (m, first + n)),
        out_shape=jax.ShapeDtypeStruct(act.shape, BF16),
        scratch_shapes=[pltpu.VMEM((dim, 2 * FF_TILE), BF16)],
        input_output_aliases={len(ops) - 1: 0},
        compiler_params=params(("arbitrary", "arbitrary")),
        cost_estimate=cost(2 * seq * dim * cols, seq * dim * 4),
        name="gate_up",
    )(*ops)


def down_kernel(plan, act_ref, *refs):
    n_w = sum(len(p) for p in plan)
    w_refs = refs[:n_w]
    out_ref, w_s, sems = refs[-3:]
    j, m = pl.program_id(0), pl.program_id(1)

    def copies(t):
        at = sum(len(p) for p in plan[:t])
        slot = t % 2
        return [pltpu.make_async_copy(w_refs[at + i], w_s.at[slot, pl.ds(row, w_refs[at + i].shape[0]), pl.ds(col, w_refs[at + i].shape[1])],
                                      sems.at[slot, i]) for i, (row, col) in enumerate(plan[t])]

    for t in range(len(plan)):
        @pl.when(jnp.logical_and(j == t, m == 0))
        def _(t=t):
            if t == 0:
                for c in copies(0):
                    c.start()
            for c in copies(t):
                c.wait()
            if t + 1 < len(plan):
                for c in copies(t + 1):
                    c.start()

    slot = lax.rem(j, 2)
    sub = 256
    for r in range(0, out_ref.shape[0], sub):
        rows = pl.ds(r, sub)
        out_ref[rows, :] = jnp.dot(act_ref[rows, :], w_s[slot], preferred_element_type=F32).astype(BF16)


def down(act, pairs, n_cols=None, first=0, buf=None):
    seq, kdim = act.shape
    blk = pairs[0][0][0].shape[1]
    tm = 512
    plan, ws = [], []
    for pair in pairs:
        spots = []
        for side, group in enumerate(pair):
            row = 0
            for p in group:
                spots.append((row, side * blk))
                ws.append(p)
                row += p.shape[0]
        plan.append(spots)
    n_cols = n_cols or 2 * blk * len(pairs)
    aliased = 0 if buf is None else 1
    ops = [act] + ws + ([buf] if aliased else [])
    return pl.pallas_call(
        functools.partial(down_kernel, plan),
        grid=(len(pairs), seq // tm),
        in_specs=[pl.BlockSpec((tm, kdim), lambda j, m: (m, 0))] + [pl.BlockSpec(memory_space=pl.ANY)] * (len(ws) + aliased),
        out_specs=pl.BlockSpec((tm, 2 * blk), lambda j, m: (m, first + j)),
        out_shape=jax.ShapeDtypeStruct((seq, n_cols), BF16),
        scratch_shapes=[pltpu.VMEM((2, kdim, 2 * blk), BF16), pltpu.SemaphoreType.DMA((2, 4))],
        input_output_aliases={len(ops) - 1: 0} if aliased else {},
        compiler_params=params(("arbitrary", "arbitrary")),
        cost_estimate=cost(2 * seq * kdim * 2 * blk * len(pairs), seq * kdim * 2),
        name="down",
    )(*ops)


def ring_kernel(n_w, *refs):
    act_ref, x_ref, w_refs, y_ref = refs[0], refs[1], refs[2:2 + n_w], refs[2 + n_w]
    act_s, w_s, part, got, total, act_sem, w_sem, send_sem, recv_sem, out_sem = refs[3 + n_w:]
    dim = x_ref.shape[1]
    chip, core = lax.axis_index("wg") // 2, lax.axis_index("wg") % 2
    n_chip = lax.axis_size("wg") // 2
    n_pairs, _, seq, blk = part.shape
    n_tp = lax.axis_size("tp")
    d = lax.axis_index("tp")
    quarter = seq // n_tp
    n_steps = 2 * (n_tp - 1)
    half_rows = act_s.shape[1]
    per = n_w // n_pairs
    k_half = w_refs[0].shape[0]

    barrier = pltpu.get_barrier_semaphore()
    for sg in (1, -1):
        pl.semaphore_signal(barrier, inc=1, device_id={"tp": lax.rem(d + sg + n_tp, n_tp)},
                            device_id_type=pl.DeviceIdType.MESH)
    pl.semaphore_wait(barrier, 2)

    def act_copy(i):
        return pltpu.make_async_copy(act_ref.at[pl.ds(i * half_rows, half_rows), :], act_s.at[i], act_sem.at[i])

    def w_copies(t):
        out = []
        for i in range(per):
            side, row = i // 2, (i % 2) * k_half
            dst = w_s.at[t % 2, pl.ds(row, k_half), pl.ds(side * blk, blk)]
            out.append(pltpu.make_async_copy(w_refs[t * per + i], dst, w_sem.at[t % 2, i]))
        return out

    def rows_of(q):
        return pl.ds(pl.multiple_of(lax.rem(q + 2 * n_tp, n_tp) * quarter, quarter), quarter)

    def ring_copy(t, side, s):
        sg = 1 - 2 * side
        if s < n_tp - 1:
            src, dst = part.at[t, side, rows_of(d - sg * s), :], got.at[t, side, s]
        else:
            rows = rows_of(d + sg * (n_tp - s))
            src, dst = total.at[t, side, rows, :], total.at[t, side, rows, :]
        return pltpu.make_async_remote_copy(
            src_ref=src, dst_ref=dst, send_sem=send_sem.at[t, side, s], recv_sem=recv_sem.at[t, side, s],
            device_id={"tp": lax.rem(d + sg + n_tp, n_tp)}, device_id_type=pl.DeviceIdType.MESH)

    def x_copy(i, first):
        return pltpu.make_async_copy(x_ref.at[pl.ds(first + i * half_rows, half_rows), :],
                                     act_s.at[i, :, pl.ds(0, dim)], act_sem.at[i])

    def place(t, side, k):
        q = lax.rem(d + (1 - 2 * side) * (1 - k) + 2 * n_tp, n_tp)
        here = lax.rem(chip + CHIP_STEPS[t] + n_chip, n_chip) * 2 + (core if side == 0 else 1 - core)
        per_half = half_rows // quarter
        return q, q // per_half, (q % per_half) * quarter, pl.multiple_of(here * blk, blk)

    def out_copy(t, side, k):
        q, h, row, col = place(t, side, k)
        src = act_s.at[h, pl.ds(pl.multiple_of(row, quarter), quarter), pl.ds(col, blk)]
        dst = y_ref.at[pl.ds(pl.multiple_of(q * quarter, quarter), quarter), pl.ds(col, blk)]
        return pltpu.make_async_copy(src, dst, out_sem.at[t, side, k])

    def finish(t, side, k):
        q, h, row, col = place(t, side, k)

        def add(i, carry):
            at = i * 128
            spot = (h, pl.ds(pl.multiple_of(row + at, 128), 128), pl.ds(col, blk))
            tot = total[t, side, pl.ds(pl.multiple_of(q * quarter + at, 128), 128), :]
            act_s[spot] = (act_s[spot].astype(F32) + tot.astype(F32)).astype(BF16)
            return carry

        lax.fori_loop(0, quarter // 128, add, 0)

    def action(t, s):
        for side in range(2):
            sg = 1 - 2 * side
            if s:
                ring_copy(t, side, s - 1).wait_recv()
            if 0 < s < n_tp:
                q = lax.rem(d - sg * s + 2 * n_tp, n_tp) * quarter
                into = part if s < n_tp - 1 else total

                def add(i, carry, side=side, q=q, into=into):
                    at = pl.multiple_of(i * 128, 128)
                    rows = pl.ds(pl.multiple_of(q + at, 128), 128)
                    into[t, side, rows, :] = (part[t, side, rows, :].astype(F32)
                                              + got[t, side, s - 1, pl.ds(at, 128), :].astype(F32)).astype(BF16)
                    return carry

                lax.fori_loop(0, quarter // 128, add, 0)
        for side in range(2):
            if s < n_steps:
                ring_copy(t, side, s).start()
        if s >= n_tp - 1:
            for side in range(2):
                finish(t, side, s - (n_tp - 1))
            for side in range(2):
                out_copy(t, side, s - (n_tp - 1)).start()

    for i in range(2):
        act_copy(i).start()
    for c in w_copies(0):
        c.start()

    def pair(t, carry):
        for tt in range(n_pairs):
            @pl.when(t == tt)
            def _(tt=tt):
                for c in w_copies(tt):
                    c.wait()
                if tt + 1 < n_pairs:
                    for c in w_copies(tt + 1):
                        c.start()
        for i in range(2):
            @pl.when(t == 0)
            def _(i=i):
                act_copy(i).wait()

            def tile(r, c2, i=i):
                at = pl.multiple_of(r * 256, 256)
                out = jnp.dot(act_s[i, pl.ds(at, 256), :], w_s[lax.rem(t, 2)], preferred_element_type=F32).astype(BF16)
                rows = pl.ds(pl.multiple_of(i * half_rows + at, 256), 256)
                part[t, 0, rows, :] = out[:, :blk]
                part[t, 1, rows, :] = out[:, blk:]
                return c2

            lax.fori_loop(0, half_rows // 256, tile, 0)

            @pl.when(t > 0)
            def _(i=i):
                action(t - 1, 1 + i)
        action(t, 0)
        return carry

    lax.fori_loop(0, n_pairs, pair, 0)
    for i in range(2):
        x_copy(i, x_ref.shape[0] - seq).start()
    for i in range(2):
        x_copy(i, x_ref.shape[0] - seq).wait()

    state = [3] * (n_pairs - 1) + [1]
    while min(state) <= n_steps:
        for t in [n_pairs - 1] + list(range(n_pairs - 1)):
            if state[t] <= n_steps and (t == n_pairs - 1 or state[t] <= state[-1] + 1):
                action(t, state[t])
                state[t] += 1

    for t in range(n_pairs):
        for side in range(2):
            for s in range(n_steps):
                ring_copy(t, side, s).wait_send()
            for k in range(n_tp):
                out_copy(t, side, k).wait()


def down_ring(act, x, pairs):
    seq, kdim = act.shape
    ws = [p for pair in pairs for group in pair for p in group]
    blk = ws[0].shape[1]
    n_pairs = len(pairs)
    n_tp = lax.axis_size("tp")
    n_steps = 2 * (n_tp - 1)
    shape = (n_pairs, 2, seq, blk)
    return pl.pallas_call(
        functools.partial(ring_kernel, len(ws)),
        in_specs=[pl.BlockSpec(memory_space=pl.ANY)] * (2 + len(ws)),
        out_specs=pl.BlockSpec(memory_space=pl.ANY),
        out_shape=jax.ShapeDtypeStruct((seq, x.shape[1]), BF16),
        scratch_shapes=[pltpu.VMEM((2, seq // 2, kdim), BF16), pltpu.VMEM((2, kdim, 2 * blk), BF16),
                        pltpu.VMEM(shape, BF16), pltpu.VMEM((n_pairs, 2, n_tp - 1, seq // n_tp, blk), BF16),
                        pltpu.VMEM(shape, BF16),
                        pltpu.SemaphoreType.DMA((2,)), pltpu.SemaphoreType.DMA((2, len(ws) // n_pairs)),
                        pltpu.SemaphoreType.DMA((n_pairs, 2, n_steps)), pltpu.SemaphoreType.DMA((n_pairs, 2, n_steps)),
                        pltpu.SemaphoreType.DMA((n_pairs, 2, n_tp))],
        compiler_params=pltpu.CompilerParams(collective_id=0, has_side_effects=True, vmem_limit_bytes=VMEM_LIMIT),
        cost_estimate=cost(1.4e11, seq * kdim * 2),
        name="down_ring",
    )(act, x, *ws)


def add_kernel(n_m, idx_ref, x_ref, *refs):
    tots, last_ref, y_ref = refs[:-2], refs[-2], refs[-1]
    blk = x_ref.shape[1] // N_PIECES

    @pl.when(pl.program_id(0) < n_m)
    def _():
        j = 0
        for t in tots:
            for c in range(0, t.shape[1], blk):
                spot = pl.ds(pl.multiple_of(idx_ref[j] * blk, blk), blk)
                y_ref[:, spot] = (x_ref[:, spot].astype(F32) + t[:, c:c + blk].astype(F32)).astype(BF16)
                j += 1

    @pl.when(pl.program_id(0) >= n_m)
    def _():
        y_ref[...] = last_ref[...]


def residual(x, totals, idx, last):
    rows, dim = x.shape
    seq = last.shape[0]
    tm = 512
    n_m = seq // tm
    first = lambda m, p: (jnp.minimum(m, n_m - 1), 0)
    return pl.pallas_call(
        functools.partial(add_kernel, n_m),
        grid_spec=pltpu.PrefetchScalarGridSpec(
            num_scalar_prefetch=1, grid=(rows // tm,),
            in_specs=[pl.BlockSpec((tm, dim), first)]
            + [pl.BlockSpec((tm, t.shape[1]), first) for t in totals]
            + [pl.BlockSpec((tm, dim), lambda m, p: (jnp.maximum(m - n_m, 0), 0))],
            out_specs=pl.BlockSpec((tm, dim), lambda m, p: (m, 0))),
        out_shape=jax.ShapeDtypeStruct((rows, dim), BF16),
        compiler_params=params(("arbitrary",)),
        cost_estimate=cost(5e9, rows * dim * 6),
        name="residual",
    )(idx, x, *totals, last)


def rope_tables(seq_len, head_dim):
    half = head_dim // 2
    inv_freq = 10000.0 ** (-2.0 * jnp.arange(half, dtype=F32) / head_dim)
    angles = jnp.arange(seq_len, dtype=F32)[:, None] * inv_freq[None, :]
    return jnp.cos(angles), jnp.sin(angles)


def solution(mesh):
    n_wg = mesh.shape['wg']
    batch_spec = P(('dp', 'wg'), None, None)
    in_specs = (batch_spec, P(('dp', 'wg'), None), P(None), P('wg', 'tp'), P('wg', None),
                P('wg', 'tp'), P('wg', 'tp'), P('tp', 'wg'), P('tp', 'wg'))
    out_specs = (batch_spec, batch_spec, batch_spec)
    to_right = [(i, (i + 2) % n_wg) for i in range(n_wg)]
    to_left = [(i, (i - 2) % n_wg) for i in range(n_wg)]
    far_right = [(i, (i + 4) % n_wg) for i in range(n_wg)]
    far_left = [(i, (i - 4) % n_wg) for i in range(n_wg)]
    to_pair = [(i, i ^ 1) for i in range(n_wg)]

    def shift(val, pairs):
        return lax.ppermute(val, 'wg', pairs)

    def halves(v):
        return v[:v.shape[0] // 2], v[v.shape[0] // 2:]

    def spread(shard):
        top, bottom = halves(shard)
        out = []
        for v, pairs in ((shard, to_right), (shard, to_left), (top, far_right), (bottom, far_left)):
            out.append(shift(v, pairs))
        return tuple(out)

    def swaps(vals):
        out = []
        for v in vals:
            out.append(shift(v, to_pair))
        return tuple(out)


    def ring_one(top, bottom):
        out = []
        for v, pairs in ((top, to_right), (bottom, to_left), (bottom, to_right), (top, to_left)):
            out.append(shift(v, pairs))
        return tuple(out)

    def ring_two(got):
        top = shift(got[0], to_right)
        bottom = shift(got[1], to_left)
        return top, bottom


    def local_step(x_in, valid, ln_gain, w_q, w_kv, w_gate, w_up, w_o, w_down):
        n_prompts, seq, dim = x_in.shape
        hd = w_kv.shape[1] // 2
        ff = w_gate.shape[1]
        me = lax.axis_index('wg')
        chip, core = me // 2, me % 2
        n_chip = n_wg // 2
        order = []
        for step in CHIP_STEPS:
            c = (chip + step + n_chip) % n_chip
            order += [2 * c + core, 2 * c + 1 - core]
        idx = jnp.stack(order).astype(jnp.int32)
        block = jnp.arange(n_wg, dtype=jnp.int32)
        away = (block // 2 - chip + n_chip) % n_chip
        slot = jnp.where(away == 0, 0, jnp.where(away == n_chip - 1, 1, jnp.where(away == 1, 2, 3)))
        pos = 2 * slot + (block % 2 != core).astype(jnp.int32)

        x2 = x_in.reshape(n_prompts * seq, dim)
        oc = w_o.shape[0]
        cut_at = 5 * FF_TILE

        def chunk(gate, up, lo, hi):
            pair = [gate[:, lo:hi], up[:, lo:hi]]
            return tuple(jnp.concatenate([halves(v)[i] for v in pair], axis=1) for i in range(2))

        def tie(vals, *deps):
            return lax.optimization_barrier(tuple(vals) + deps)[:len(vals)]

        def k_pieces(own, got):
            sw = swaps((own,) + got)
            return [own, sw[0], got[0], sw[1], got[1], sw[2], got[2], got[3], sw[3], sw[4]]

        def ring_pieces(near, sw_near, far, sw_far):
            out = []
            for i, j in ((0, 1), (2, 4), (5, 3)):
                out += [near[i], near[j], sw_near[i], sw_near[j]]
            return out + list(far) + list(sw_far)

        s_q = jnp.concatenate([w_q, w_kv], axis=1)
        got_q = spread(s_q)
        cos_t, sin_t = rope_tables(seq, hd)
        valid_col = valid.reshape(-1, 1)
        valid_row = valid.reshape(n_prompts, 1, seq)

        z0 = layer_norm(after(x2, s_q), ln_gain, pos, 0, seq)
        s_a = chunk(*tie([w_gate, w_up], z0), 0, cut_at)
        one_a = ring_one(*s_a)
        got_q = tie(got_q, *s_a)
        p_q = k_pieces(s_q, got_q)
        z1 = layer_norm(after(x2, *got_q), ln_gain, pos, 1, seq)
        s_b = chunk(*tie([w_gate, w_up], z1), cut_at, ff)
        q0, k_cache, v_cache, v0 = qkv(after(z0, *s_b), p_q, cos_t, sin_t, valid_col, hd, 0, ())
        act0 = attention(q0, k_cache, v0, valid_row, 0, oc + ff)

        near_a = tie(s_a + one_a, act0)
        far_a = ring_two(near_a[2:])
        sw_near = swaps(near_a)
        q1, k_cache, v_cache, v1 = qkv(after(z1, *near_a), p_q, cos_t, sin_t, valid_col, hd, 1,
                                          (k_cache, v_cache))
        s_b = tie(s_b, q1)
        one_b = ring_one(*s_b)
        act1 = attention(after(q1, *s_b), k_cache, v1, valid_row, 1, oc + ff)
        far_a = tie(far_a, act1)
        p_a = ring_pieces(near_a, sw_near, far_a, swaps(far_a))
        act0 = gate_up(z0, p_a, act0, oc, 0, 3)

        near_b = tie(s_b + one_b, act0)
        far_b = ring_two(near_b[2:])
        sw_near = swaps(near_b)
        act0 = gate_up(z0, p_a, after(act0, *near_b), oc, 3, None)
        top_d, bottom_d = tie(halves(jnp.concatenate(tie([w_o, w_down], q1), axis=0)), act0)
        one_d = ring_one(top_d, bottom_d)
        far_b = tie(far_b, act0)
        p_b = ring_pieces(near_b, sw_near, far_b, swaps(far_b))
        own_d = swaps((top_d, bottom_d))
        act0 = gate_up(z0, p_b, act0, oc + cut_at)

        pair_0 = ([top_d, bottom_d], list(own_d))
        part_a = down(act0, [pair_0])
        tot_a = lax.psum(part_a, 'tp')
        one_d = tie(one_d, part_a)
        far_d = ring_two(one_d)
        sw_near = swaps(one_d)
        near = [([one_d[0], one_d[2]], [sw_near[0], sw_near[2]]), ([one_d[3], one_d[1]], [sw_near[3], sw_near[1]])]
        part_b = down(after(act0, *one_d), near, dim - part_a.shape[1])
        far_d = tie(far_d, part_b)
        sw_far = swaps(far_d)
        pair_3 = (list(far_d), list(sw_far))
        part_b = down(act0, [pair_3], dim - part_a.shape[1], 2, part_b)
        tot_b = lax.psum(after(part_b, tot_a), 'tp')

        act1 = gate_up(z1, p_a, after(act1, part_b), oc)
        act1 = gate_up(z1, p_b, act1, oc + cut_at)
        y_last = down_ring(act1, x2, [pair_0] + near + [pair_3])

        y = residual(x2, [tot_a, tot_b], idx, y_last)
        out3 = lambda v: v.reshape(n_prompts, seq, v.shape[-1])
        return out3(y), out3(k_cache), out3(v_cache)

    return jax.shard_map(local_step, mesh=mesh, in_specs=in_specs, out_specs=out_specs, check_vma=False)
```
